32 devices in a mesh: gx: 4 (over z), gy: 4 (over x, core), gz: 2 (over y).
Axes of the slice: x: 2, y: 2, z: 4, core: 2. Of those that a mesh axis runs over, the one named last changes fastest.
Arguments:
- right_side: float32 [256, 256, 512], P('gx', 'gy', 'gz'), may hold values from -6 to 6
- guess: float32 [256, 256, 512], P('gx', 'gy', 'gz'), may hold values from -4 to 4
Outputs:
- updated: float32 [256, 256, 512], P('gx', 'gy', 'gz')
- new_residual: float32 [256, 256, 512], P('gx', 'gy', 'gz')
- res_norm: float32 [], replicated
The draws below stay inside these ranges and needn't reach their ends.
All inputs are finite; a program needn't handle non-finite values.
Results may differ from the reference program's by a relative error of at most 0.0003.
Values sent between devices are 32-bit elements; how exact they have to be, the bound alone decides.
A program may use at most 128 MiB of HBM per device.

```python
import math
import jax
import jax.numpy as jnp

COARSEN = 4
NX = 256
NY = 256
NZ = 512


def level_of(stream_key, shape, pieces, low, top_value):
    loudness = 1.0
    for dim, blocks in pieces:
        heights = jax.random.uniform(jax.random.fold_in(jax.random.fold_in(stream_key, 6), dim), (blocks,), jnp.float32, low / len(pieces), top_value / len(pieces))
        loudness = loudness * jnp.repeat(jnp.exp(heights), shape[dim] // blocks).reshape((-1,) + (1,) * (len(shape) - 1 - dim))
    return loudness


def scatter_about(stream_key, extent, width, reach, pieces=(), kind=jnp.bfloat16):
    array = jax.random.normal(stream_key, extent, jnp.float32) * width
    if len(pieces) > 0:
        array = level_of(stream_key, extent, pieces, -0.22, 0.18) * array
    return jnp.clip(array, min=-reach, max=reach).astype(kind)


def setup_inputs(seed: int = 0) -> dict:
    seeds = jax.random.split(jax.random.key(seed), 3)
    return {
        "right_side": scatter_about(seeds[0], (NX, NY, NZ), 1.0, 6.0, ((0, 4), (1, 4), (2, 2)), jnp.float32),
        "guess": scatter_about(seeds[1], (NX, NY, NZ), 0.5, 4.0, ((0, 4), (1, 4), (2, 2)), jnp.float32),
    }


screen = 0.002

def neighbours(values):
    total = jnp.roll(values, 1, 0) + jnp.roll(values, -1, 0)
    total = total + jnp.roll(values, 1, 1) + jnp.roll(values, -1, 1)
    total = total + jnp.roll(values, 1, 2) + jnp.roll(values, -1, 2)
    return total

def apply_operator(values):
    return (6.0 + screen) * values - neighbours(values)

def eigen_line(length):
    index = jnp.arange(length, dtype=jnp.int32).astype(jnp.float32)
    return (2.0 - 2.0 * jnp.cos(2.0 * math.pi * index / length)) / (COARSEN * COARSEN)

def reference(right_side, guess):
    diag_value = 6.0 + screen
    residual_now = right_side - apply_operator(guess)
    first_sweep = residual_now / diag_value
    local_fix = (residual_now + neighbours(first_sweep)) / diag_value
    coarse_x = NX // COARSEN
    coarse_y = NY // COARSEN
    coarse_z = NZ // COARSEN
    coarse = residual_now.reshape(coarse_x, COARSEN, coarse_y, COARSEN, coarse_z, COARSEN).mean(axis=(1, 3, 5))
    eigen_sum = screen + eigen_line(coarse_x)[:, None, None] + eigen_line(coarse_y)[None, :, None] + eigen_line(coarse_z)[None, None, :]
    spectrum = jnp.fft.fftn(coarse)
    correction = jnp.real(jnp.fft.ifftn(spectrum / eigen_sum)).astype(jnp.float32)
    prolonged = jnp.repeat(jnp.repeat(jnp.repeat(correction, COARSEN, 0), COARSEN, 1), COARSEN, 2)
    updated = guess + local_fix + prolonged
    new_residual = right_side - apply_operator(updated)
    res_norm = jnp.sqrt(jnp.sum(new_residual * new_residual))
    return (updated, new_residual, res_norm)
```

```python
import functools

import jax
import jax.numpy as jnp
import numpy as np
from jax import lax
from jax.experimental import pallas as pl
from jax.experimental.pallas import tpu as pltpu
from jax.sharding import PartitionSpec as P

COARSEN = 4
SCREEN = 0.002
DIAG = 6.0 + SCREEN
LANES = 128
EXACT = lax.Precision.HIGHEST
MESH = pl.DeviceIdType.MESH


def cas(length):
    index = np.arange(length)
    angle = 2.0 * np.pi * (np.outer(index, index) % length) / length
    return np.cos(angle) + np.sin(angle)


def eigen_line(length):
    index = np.arange(length)
    return (2.0 - 2.0 * np.cos(2.0 * np.pi * index / length)) / (COARSEN * COARSEN)


class Plan:
    def __init__(self, counts, block):
        self.px, self.py, self.pz = counts
        self.bx, self.by, self.bz = block
        self.ndev = self.px * self.py * self.pz
        self.group = self.py * self.pz
        self.cx, self.cy, self.cz = (n // COARSEN for n in block)
        self.lx, self.ly, self.lz = self.cx * self.px, self.cy * self.py, self.cz * self.pz
        self.rx = self.cx // self.group
        self.rk = self.ly // self.ndev
        assert self.rx * self.group == self.cx and self.rk * self.ndev == self.ly
        self.rows = self.rx * self.rk
        self.hr = -(-(self.cy + 2) // 8) * 8

    def tables(self):
        px, py, pz, group, ndev = self.px, self.py, self.pz, self.group, self.ndev
        cx, cy, cz, rx, rk = self.cx, self.cy, self.cz, self.rx, self.rk
        lx, ly, lz, hr = self.lx, self.ly, self.lz, self.hr
        tx, ty, tz = cas(lx), cas(ly), cas(lz)
        up_z = np.arange(self.bz) // COARSEN
        mz = np.stack([tz[g * cz + up_z] for g in range(pz)]) / COARSEN**3
        pool = (np.arange(self.by)[None, :] // COARSEN == np.arange(cy)[:, None]) * 1.0
        my = np.zeros((ndev, rx, rk, py, pz, rx, cy))
        for j in range(rx):
            part = ty.reshape(py, cy, ndev, rk).transpose(2, 3, 0, 1)
            my[:, j, :, :, :, j, :] = part[:, :, :, None, :]
        my = my.reshape(ndev * rx * rk, group * rx * cy)
        mx = np.zeros((rk, lx, px, group, rx, rk))
        for k in range(rk):
            mx[k, :, :, :, :, k] = tx.reshape(px, group, rx, lx).transpose(3, 0, 1, 2)
        mx = mx.reshape(rk * lx, ndev * rx * rk)
        mxi = mx.T / (lx * ly * lz)
        rows_of = np.arange(py)[:, None] * cy + np.concatenate([np.arange(cy), [-1, cy]])[None, :]
        lines = np.zeros((py, hr, ly))
        lines[:, : cy + 2] = ty[rows_of % ly]
        myi = np.zeros((py, rx, hr, ndev, rx, rk))
        for j in range(rx):
            myi[:, j, :, :, j, :] = lines.reshape(py, hr, ndev, rk)
        myi = myi.reshape(py * rx * hr, ndev * rx * rk)
        mzi = np.zeros((pz, lz, self.bz + LANES))
        for g in range(pz):
            mzi[g, :, : self.bz] = tz[:, g * cz + up_z]
            mzi[g, :, self.bz] = tz[:, (g * cz - 1) % lz]
            mzi[g, :, self.bz + LANES - 1] = tz[:, (g * cz + cz) % lz]
        spread = (np.arange(self.by)[:, None] // COARSEN == np.arange(hr)[None, :]) * 1.0
        ei = SCREEN + eigen_line(lx)[:, None] + eigen_line(lz)[None, :]
        ey = np.repeat(eigen_line(ly)[:, None, None], lz, axis=2)
        return [t.astype(np.float32) for t in (mz, pool, my, mx, mxi, myi, mzi, spread, ei, ey)]


def dot(a, b):
    return jnp.dot(a, b, precision=EXACT, preferred_element_type=jnp.float32)


def kernel(plan, rs_hbm, g_hbm, *refs):
    q = plan
    table_hbm = refs[:10]
    up_hbm, res_hbm, norm_out = refs[10:13]
    tabs = refs[13:23]
    mz, pool, my, mx, mxi, myi, mzi, spread, ei, ey = tabs
    (rs, g, r, u, n, yp, zp, yh, zh, pooled, first, r1, s2, r2, flat, s3, r3, s4, r4, zf, wz, nrm,
     in_sem, tab_sem, out_sem, face_send, face_recv, a_send, a_recv) = refs[23:]
    ndev, group = q.ndev, q.group
    bx, by, bz = q.bx, q.by, q.bz
    ix, iy, iz = lax.axis_index("gx"), lax.axis_index("gy"), lax.axis_index("gz")
    me_p = iy * q.pz + iz
    me = ix * group + me_p

    def coords(lin):
        return (lin // group, (lin % group) // q.pz, lin % q.pz)

    in_chunks = 4
    step = bx // in_chunks
    copies_g = [
        pltpu.make_async_copy(g_hbm.at[pl.ds(c * step, step)], g.at[pl.ds(1 + c * step, step)], in_sem.at[c])
        for c in range(in_chunks)
    ]
    copies_r = [
        pltpu.make_async_copy(rs_hbm.at[pl.ds(c * step, step)], rs.at[pl.ds(c * step, step)], in_sem.at[in_chunks + c])
        for c in range(in_chunks)
    ]
    copies_t = [pltpu.make_async_copy(a, b, tab_sem.at[i]) for i, (a, b) in enumerate(zip(table_hbm, tabs))]
    for c in copies_g + copies_r + copies_t:
        c.start()

    barrier = pltpu.get_barrier_semaphore()

    def greet(k, carry):
        pl.semaphore_signal(barrier, inc=1, device_id=coords((me + k) % ndev), device_id_type=MESH)
        return carry

    lax.fori_loop(1, ndev, greet, 0)

    lane = lax.broadcasted_iota(jnp.int32, (by, LANES), 1)
    row = lax.broadcasted_iota(jnp.int32, (by, LANES), 0)

    def pack_plane(x, v, phase, acc):
        lo, hi = acc
        yp[phase, 0, x] = v[0:1, :]
        yp[phase, 1, x] = v[by - 1 : by, :]
        lo = jnp.where(lane == x, pltpu.roll(v[:, :LANES], x, 1), lo)
        hi = jnp.where(lane == x, pltpu.roll(v[:, bz - LANES :], (x + 1) % LANES, 1), hi)
        return lo, hi

    zero_acc = (jnp.zeros((by, LANES), jnp.float32), jnp.zeros((by, LANES), jnp.float32))

    def face_copies(phase, buf):
        xl, xr = (ix + q.px - 1) % q.px, (ix + 1) % q.px
        yl, yr = (iy + q.py - 1) % q.py, (iy + 1) % q.py
        zl, zr = (iz + q.pz - 1) % q.pz, (iz + 1) % q.pz
        moves = [
            (buf.at[1], buf.at[bx + 1], (xl, iy, iz)),
            (buf.at[bx], buf.at[0], (xr, iy, iz)),
            (yp.at[phase, 0], yh.at[phase, 1], (ix, yl, iz)),
            (yp.at[phase, 1], yh.at[phase, 0], (ix, yr, iz)),
            (zp.at[phase, 0], zh.at[phase, 1], (ix, iy, zl)),
            (zp.at[phase, 1], zh.at[phase, 0], (ix, iy, zr)),
        ]
        return [
            pltpu.make_async_remote_copy(
                src_ref=s, dst_ref=d, send_sem=face_send.at[phase, i], recv_sem=face_recv.at[phase, i],
                device_id=dev, device_id_type=MESH,
            )
            for i, (s, d, dev) in enumerate(moves)
        ]

    def plane_sum(x, buf, phase, ylo, yhi, zadd):
        v = buf[x + 1]
        zlo = pltpu.roll(zh[phase, 0], (LANES - x) % LANES, 1)
        zhi = pltpu.roll(zh[phase, 1], LANES - 1 - x, 1)
        if zadd is not None:
            zlo, zhi = zlo + zadd, zhi + zadd
        tiles = [v[:, t * LANES : (t + 1) * LANES] for t in range(bz // LANES)]
        up = [pltpu.roll(t, 1, 1) for t in tiles]
        down = [pltpu.roll(t, LANES - 1, 1) for t in tiles]
        out = []
        for t, c in enumerate(tiles):
            cols = slice(t * LANES, (t + 1) * LANES)
            total = buf[x, :, cols] + buf[x + 2, :, cols]
            total += jnp.where(row == 0, ylo[:, cols], pltpu.roll(c, 1, 0))
            total += jnp.where(row == by - 1, yhi[:, cols], pltpu.roll(c, by - 1, 0))
            total += jnp.where(lane == 0, up[t - 1] if t > 0 else zlo, up[t])
            total += jnp.where(lane == LANES - 1, down[t + 1] if t + 1 < len(tiles) else zhi, down[t])
            out.append(total)
        return v, jnp.concatenate(out, axis=1)

    for c in copies_g:
        c.wait()
    lo, hi = lax.fori_loop(0, bx, lambda x, acc: pack_plane(x, g[x + 1], 0, acc), zero_acc, unroll=4)
    zp[0, 0], zp[0, 1] = lo, hi
    pl.semaphore_wait(barrier, ndev - 1)
    faces0 = face_copies(0, g)
    for c in faces0:
        c.start()
    for c in copies_r:
        c.wait()
    for c in faces0:
        c.wait_recv()

    def residual_four(i, acc):
        total = jnp.zeros((by, bz), jnp.float32)
        for a in range(COARSEN):
            x = i * COARSEN + a
            v, around = plane_sum(x, g, 0, yh[0, 0, x], yh[0, 1, x], None)
            res = rs[x] - (DIAG * v - around)
            r[x + 1] = res
            total += res
            acc = pack_plane(x, res, 1, acc)
        pooled[i] = total
        return acc

    lo, hi = lax.fori_loop(0, q.cx, residual_four, zero_acc)
    zp[1, 0], zp[1, 1] = lo, hi
    for c in copies_t:
        c.wait()

    def fold_rows(i, carry):
        zf[i, : q.cy, :bz] = dot(pool[...], pooled[i])
        return carry

    lax.fori_loop(0, q.cx, fold_rows, 0, unroll=True)
    cells = zf[: q.cx, : q.cy, :bz].reshape(q.cx * q.cy, bz)
    first[...] = dot(cells, mz[iz]).reshape(first.shape)

    def spread_out(src, dst, stage, peers, here, device_of, own):
        def send(k, carry):
            d = (here + k) % peers
            pltpu.make_async_remote_copy(
                src_ref=src.at[d], dst_ref=dst.at[here], send_sem=a_send.at[stage], recv_sem=a_recv.at[stage],
                device_id=device_of(d), device_id_type=MESH,
            ).start()
            return carry

        lax.fori_loop(1, peers, send, 0)
        dst[here] = own

    def all_bytes(dst, count, sem):
        part = dst.at[pl.ds(0, count)]
        pltpu.make_async_copy(part, part, sem).wait()

    in_group = lambda d: (ix, d // q.pz, d % q.pz)
    spread_out(first, r1, 0, group, me_p, in_group, first[me_p])
    faces1 = face_copies(1, r)
    for c in faces1:
        c.start()

    def fix_planes(start, stop, acc):
        def body(x, acc):
            v, around = plane_sum(x, r, 1, yh[1, 0, x], yh[1, 1, x], None)
            out = g[x + 1] + (v + around * (1.0 / DIAG)) * (1.0 / DIAG)
            u[x + 1] = out
            return pack_plane(x, out, 2, acc)

        return lax.fori_loop(start, stop, body, acc, unroll=2)

    all_bytes(r1, group - 1, a_recv.at[0])
    lines = dot(my[...], r1[...].reshape(group * q.rx * q.cy, q.lz))
    for d in range(ndev):
        s2[d] = lines[d * q.rows : (d + 1) * q.rows]
    spread_out(s2, r2, 1, ndev, me, coords, s2[me])
    for c in faces1:
        c.wait_recv()
    acc = fix_planes(0, bx // 2, zero_acc)
    all_bytes(r2, ndev - 1, a_recv.at[1])
    for d in range(ndev):
        flat[d * q.rows : (d + 1) * q.rows] = r2[d]
    spec = dot(mx[...], flat[...])
    spec = jnp.concatenate(
        [spec[k * q.lx : (k + 1) * q.lx] / (ei[...] + ey[me * q.rk + k]) for k in range(q.rk)], axis=0
    )
    lines = dot(mxi[...], spec)
    for d in range(ndev):
        s3[d] = lines[d * q.rows : (d + 1) * q.rows]
    spread_out(s3, r3, 2, ndev, me, coords, s3[me])
    lo, hi = fix_planes(bx // 2, bx, acc)
    zp[2, 0], zp[2, 1] = lo, hi
    faces2 = face_copies(2, u)
    for c in faces2:
        c.start()
    all_bytes(r3, ndev - 1, a_recv.at[2])
    for d in range(ndev):
        flat[d * q.rows : (d + 1) * q.rows] = r3[d]
    s4[...] = dot(myi[...], flat[...]).reshape(s4.shape)

    def send_lines(k, carry):
        d = (me_p + k) % group
        pltpu.make_async_remote_copy(
            src_ref=s4.at[d // q.pz], dst_ref=r4.at[pl.ds(me_p * q.rx, q.rx)],
            send_sem=a_send.at[3], recv_sem=a_recv.at[3], device_id=in_group(d), device_id_type=MESH,
        ).start()
        return carry

    lax.fori_loop(1, group, send_lines, 0)
    r4[pl.ds(me_p * q.rx, q.rx)] = s4[iy]

    def edge(to_x, j, slot, sem):
        def send(d, carry):
            pltpu.make_async_remote_copy(
                src_ref=s4.at[d // q.pz, j], dst_ref=r4.at[slot], send_sem=a_send.at[sem], recv_sem=a_recv.at[sem],
                device_id=(to_x, d // q.pz, d % q.pz), device_id_type=MESH,
            ).start()
            return carry

        lax.fori_loop(0, group, send, 0)

    @pl.when(me_p == group - 1)
    def _():
        edge((ix + 1) % q.px, q.rx - 1, q.cx, 4)

    @pl.when(me_p == 0)
    def _():
        edge((ix + q.px - 1) % q.px, 0, q.cx + 1, 5)

    all_bytes(r4, (group - 1) * q.rx, a_recv.at[3])
    all_bytes(r4, 1, a_recv.at[4])
    all_bytes(r4, 1, a_recv.at[5])
    zf[...] = dot(r4[...].reshape((q.cx + 2) * q.hr, q.lz), mzi[iz]).reshape(zf.shape)

    def prolong(i, carry):
        fine = dot(spread[...], zf[i])
        wz[i] = fine[:, bz:]
        for a in range(COARSEN):
            u[1 + i * COARSEN + a] += fine[:, :bz]
        return carry

    for c in faces2:
        c.wait_send()
    lax.fori_loop(0, q.cx, prolong, 0)
    out_u = pltpu.make_async_copy(u.at[pl.ds(1, bx)], up_hbm, out_sem.at[0])
    out_u.start()
    for c in faces2:
        c.wait_recv()
    u[0] += dot(spread[...], zf[q.cx])[:, :bz]
    u[bx + 1] += dot(spread[...], zf[q.cx + 1])[:, :bz]

    out_planes = bx // in_chunks
    outs_n = []
    total = jnp.zeros((by, bz), jnp.float32)
    for c in range(in_chunks):

        def last_four(i, total):
            ylo, yhi = zf[i, q.cy : q.cy + 1, :bz], zf[i, q.cy + 1 : q.cy + 2, :bz]
            for a in range(COARSEN):
                x = i * COARSEN + a
                v, around = plane_sum(x, u, 2, yh[2, 0, x] + ylo, yh[2, 1, x] + yhi, wz[i])
                res = rs[x] - (DIAG * v - around)
                n[x] = res
                total += res * res
            return total

        total = lax.fori_loop(c * q.cx // in_chunks, (c + 1) * q.cx // in_chunks, last_four, total)
        cp = pltpu.make_async_copy(
            n.at[pl.ds(c * out_planes, out_planes)], res_hbm.at[pl.ds(c * out_planes, out_planes)], out_sem.at[1 + c]
        )
        cp.start()
        outs_n.append(cp)

    line = jnp.sum(total, axis=0, keepdims=True)
    part = line[:, :LANES]
    for t in range(1, bz // LANES):
        part = part + line[:, t * LANES : (t + 1) * LANES]
    nrm[me] = part

    def send_norm(k, carry):
        d = (me + k) % ndev
        pltpu.make_async_remote_copy(
            src_ref=nrm.at[me], dst_ref=nrm.at[me], send_sem=a_send.at[6], recv_sem=a_recv.at[6],
            device_id=coords(d), device_id_type=MESH,
        ).start()
        return carry

    lax.fori_loop(1, ndev, send_norm, 0)
    all_bytes(nrm, ndev - 1, a_recv.at[6])
    norm_out[...] = jnp.sqrt(jnp.sum(jnp.sum(nrm[...], axis=0), axis=1, keepdims=True)).reshape(1, 1)

    all_bytes(nrm, ndev - 1, a_send.at[6])
    all_bytes(first, group - 1, a_send.at[0])
    all_bytes(s2, ndev - 1, a_send.at[1])
    all_bytes(s3, ndev - 1, a_send.at[2])
    all_bytes(r4, (group - 1) * q.rx, a_send.at[3])

    @pl.when(me_p == group - 1)
    def _():
        all_bytes(r4, group, a_send.at[4])

    @pl.when(me_p == 0)
    def _():
        all_bytes(r4, group, a_send.at[5])

    for c in faces0 + faces1:
        c.wait_send()
    out_u.wait()
    for cp in outs_n:
        cp.wait()


def per_device(right_side, guess):
    counts = tuple(lax.axis_size(a) for a in ("gx", "gy", "gz"))
    q = Plan(counts, guess.shape)
    assert q.lz == LANES and q.bx <= LANES and q.bz % LANES == 0
    tables = q.tables()
    f32 = jnp.float32
    bx, by, bz = guess.shape
    vm = lambda *shape: pltpu.VMEM(shape, f32)
    scratch = [vm(*t.shape) for t in tables] + [
        vm(bx, by, bz), vm(bx + 2, by, bz), vm(bx + 2, by, bz), vm(bx + 2, by, bz), vm(bx, by, bz),
        vm(3, 2, bx, 1, bz), vm(3, 2, by, LANES), vm(3, 2, bx, 1, bz), vm(3, 2, by, LANES),
        vm(q.cx, by, bz),
        vm(q.group, q.rx, q.cy, q.lz), vm(q.group, q.rx, q.cy, q.lz),
        vm(q.ndev, q.rows, q.lz), vm(q.ndev, q.rows, q.lz), vm(q.ndev * q.rows, q.lz),
        vm(q.ndev, q.rows, q.lz), vm(q.ndev, q.rows, q.lz),
        vm(q.py, q.rx, q.hr, q.lz), vm(q.cx + 2, q.hr, q.lz),
        vm(q.cx + 2, q.hr, bz + LANES), vm(q.cx, by, LANES), vm(q.ndev, 1, LANES),
        pltpu.SemaphoreType.DMA((8,)), pltpu.SemaphoreType.DMA((len(tables),)), pltpu.SemaphoreType.DMA((5,)),
        pltpu.SemaphoreType.DMA((3, 6)), pltpu.SemaphoreType.DMA((3, 6)),
        pltpu.SemaphoreType.DMA((7,)), pltpu.SemaphoreType.DMA((7,)),
    ]
    updated, new_residual, norm = pl.pallas_call(
        functools.partial(kernel, q),
        out_shape=[
            jax.ShapeDtypeStruct(guess.shape, f32),
            jax.ShapeDtypeStruct(guess.shape, f32),
            jax.ShapeDtypeStruct((1, 1), f32),
        ],
        in_specs=[pl.BlockSpec(memory_space=pl.ANY)] * (2 + len(tables)),
        out_specs=[
            pl.BlockSpec(memory_space=pl.ANY),
            pl.BlockSpec(memory_space=pl.ANY),
            pl.BlockSpec(memory_space=pltpu.VMEM),
        ],
        scratch_shapes=scratch,
        compiler_params=pltpu.CompilerParams(
            collective_id=0, has_side_effects=True, vmem_limit_bytes=60 * 1024 * 1024
        ),
        name="schwarz_step",
    )(right_side, guess, *[jnp.asarray(t) for t in tables])
    return updated, new_residual, norm[0, 0]


def solution(mesh):
    return jax.shard_map(
        per_device,
        mesh=mesh,
        in_specs=(P("gx", "gy", "gz"), P("gx", "gy", "gz")),
        out_specs=(P("gx", "gy", "gz"), P("gx", "gy", "gz"), P()),
        check_vma=False,
    )
```

```python
import functools

import jax
import jax.numpy as jnp
import numpy as np
from jax import lax
from jax.experimental import pallas as pl
from jax.experimental.pallas import tpu as pltpu
from jax.sharding import PartitionSpec as P

COARSEN = 4
SCREEN = 0.002
DIAG = 6.0 + SCREEN
LANES = 128
EXACT = lax.Precision.HIGHEST
MESH = pl.DeviceIdType.MESH


def cas(length):
    index = np.arange(length)
    angle = 2.0 * np.pi * (np.outer(index, index) % length) / length
    return np.cos(angle) + np.sin(angle)


def eigen_line(length):
    index = np.arange(length)
    return (2.0 - 2.0 * np.cos(2.0 * np.pi * index / length)) / (COARSEN * COARSEN)


class Plan:
    def __init__(self, counts, block):
        self.px, self.py, self.pz = counts
        self.bx, self.by, self.bz = block
        self.ndev = self.px * self.py * self.pz
        self.group = self.py * self.pz
        self.cx, self.cy, self.cz = (n // COARSEN for n in block)
        self.lx, self.ly, self.lz = self.cx * self.px, self.cy * self.py, self.cz * self.pz
        self.rx = self.cx // self.group
        self.rk = self.ly // self.ndev
        assert self.rx * self.group == self.cx and self.rk * self.ndev == self.ly
        self.rows = self.rx * self.rk
        self.hr = -(-(self.cy + 2) // 8) * 8

    def tables(self):
        px, py, pz, group, ndev = self.px, self.py, self.pz, self.group, self.ndev
        cx, cy, cz, rx, rk = self.cx, self.cy, self.cz, self.rx, self.rk
        lx, ly, lz, hr = self.lx, self.ly, self.lz, self.hr
        tx, ty, tz = cas(lx), cas(ly), cas(lz)
        up_z = np.arange(self.bz) // COARSEN
        mz = np.stack([tz[g * cz + up_z] for g in range(pz)]) / COARSEN**3
        pool = (np.arange(self.by)[None, :] // COARSEN == np.arange(cy)[:, None]) * 1.0
        my = np.zeros((ndev, rx, rk, py, pz, rx, cy))
        for j in range(rx):
            part = ty.reshape(py, cy, ndev, rk).transpose(2, 3, 0, 1)
            my[:, j, :, :, :, j, :] = part[:, :, :, None, :]
        my = my.reshape(ndev * rx * rk, group * rx * cy)
        mx = np.zeros((rk, lx, px, group, rx, rk))
        for k in range(rk):
            mx[k, :, :, :, :, k] = tx.reshape(px, group, rx, lx).transpose(3, 0, 1, 2)
        mx = mx.reshape(rk * lx, ndev * rx * rk)
        mxi = mx.T / (lx * ly * lz)
        rows_of = np.arange(py)[:, None] * cy + np.concatenate([np.arange(cy), [-1, cy]])[None, :]
        lines = np.zeros((py, hr, ly))
        lines[:, : cy + 2] = ty[rows_of % ly]
        myi = np.zeros((py, rx, hr, ndev, rx, rk))
        for j in range(rx):
            myi[:, j, :, :, j, :] = lines.reshape(py, hr, ndev, rk)
        myi = myi.reshape(py * rx * hr, ndev * rx * rk)
        fine_z = np.arange(self.bz * pz) // COARSEN
        own, around = tz[:, fine_z], tz[:, np.roll(fine_z, 1)] + tz[:, np.roll(fine_z, -1)]
        mzi = np.stack([m[:, g * self.bz : (g + 1) * self.bz] for g in range(pz) for m in (own, around)])
        ei = SCREEN + eigen_line(lx)[:, None] + eigen_line(lz)[None, :]
        ey = np.repeat(eigen_line(ly)[:, None, None], lz, axis=2)
        return [t.astype(np.float32) for t in (mz, pool, my, mx, mxi, myi, mzi, ei, ey)]


def dot(a, b):
    return jnp.dot(a, b, precision=EXACT, preferred_element_type=jnp.float32)


def kernel(plan, rs_hbm, g_hbm, *refs):
    q = plan
    table_hbm = refs[:9]
    up, n, norm_out = refs[9:12]
    tabs = refs[12:21]
    mz, pool, my, mx, mxi, myi, mzi, ei, ey = tabs
    (rs, g, r, u, yp, zp, yh, zh, pooled, rows16, first, r1, s2, r2, flat, s3, r3, s4, r4, zf, zs, co, nrm,
     in_sem, tab_sem, face_send, face_recv, a_send, a_recv) = refs[21:]
    ndev, group = q.ndev, q.group
    bx, by, bz = q.bx, q.by, q.bz
    ix, iy, iz = lax.axis_index("gx"), lax.axis_index("gy"), lax.axis_index("gz")
    me_p = iy * q.pz + iz
    me = ix * group + me_p

    def coords(lin):
        return (lin // group, (lin % group) // q.pz, lin % q.pz)

    in_chunks = 4
    step = bx // in_chunks
    copies_g = [
        pltpu.make_async_copy(g_hbm.at[pl.ds(c * step, step)], g.at[pl.ds(1 + c * step, step)], in_sem.at[c])
        for c in range(in_chunks)
    ]
    copies_r = [
        pltpu.make_async_copy(rs_hbm.at[pl.ds(c * step, step)], rs.at[pl.ds(c * step, step)], in_sem.at[in_chunks + c])
        for c in range(in_chunks)
    ]
    copies_t = [pltpu.make_async_copy(a, b, tab_sem.at[i]) for i, (a, b) in enumerate(zip(table_hbm, tabs))]
    for c in copies_g + copies_r + copies_t:
        c.start()

    barrier = pltpu.get_barrier_semaphore()

    def greet(k, carry):
        pl.semaphore_signal(barrier, inc=1, device_id=coords((me + k) % ndev), device_id_type=MESH)
        return carry

    lax.fori_loop(1, ndev, greet, 0)

    lane = lax.broadcasted_iota(jnp.int32, (by, LANES), 1)
    row = lax.broadcasted_iota(jnp.int32, (by, LANES), 0)

    def pack_plane(x, v, phase, acc):
        yp[phase, 0, x] = v[0:1, :]
        yp[phase, 1, x] = v[by - 1 : by, :]
        acc = pltpu.roll(acc, LANES - 2, 1)
        return jnp.where(lane == 0, v[:, :LANES], jnp.where(lane == LANES - 1, v[:, bz - LANES :], acc))

    def unpack_start(phase):
        left, right = zh[phase, 0], zh[phase, 0 if q.pz == 2 else 1]
        left = pltpu.roll(left, (2 * bx - 1) % LANES, 1)
        right = pltpu.roll(right, (2 * bx - 3) % LANES, 1)
        return jnp.where(lane % 2 == 0, left, right)

    def unpack_next(sides):
        return pltpu.roll(sides, LANES - 2, 1)

    zero_acc = jnp.zeros((by, LANES), jnp.float32)

    def face_copies(phase, buf):
        xl, xr = (ix + q.px - 1) % q.px, (ix + 1) % q.px
        yl, yr = (iy + q.py - 1) % q.py, (iy + 1) % q.py
        zl, zr = (iz + q.pz - 1) % q.pz, (iz + 1) % q.pz
        moves = [
            (buf.at[1], buf.at[bx + 1], (xl, iy, iz)),
            (buf.at[bx], buf.at[0], (xr, iy, iz)),
            (yp.at[phase, 0], yh.at[phase, 1], (ix, yl, iz)),
            (yp.at[phase, 1], yh.at[phase, 0], (ix, yr, iz)),
            (zp.at[phase], zh.at[phase, 0], (ix, iy, zr)),
            (zp.at[phase], zh.at[phase, 1], (ix, iy, zl)),
        ]
        if q.pz == 2:
            moves.pop()
        return [
            pltpu.make_async_remote_copy(
                src_ref=s, dst_ref=d, send_sem=face_send.at[phase, i], recv_sem=face_recv.at[phase, i],
                device_id=dev, device_id_type=MESH,
            )
            for i, (s, d, dev) in enumerate(moves)
        ]

    def plane_sum(x, buf, phase, sides):
        v = buf[x + 1]
        ylo, yhi = yh[phase, 0, x], yh[phase, 1, x]
        tiles = [v[:, t * LANES : (t + 1) * LANES] for t in range(bz // LANES)]
        shift_up = [pltpu.roll(t, 1, 1) for t in tiles]
        down = [pltpu.roll(t, LANES - 1, 1) for t in tiles]
        out = []
        for t, c in enumerate(tiles):
            cols = slice(t * LANES, (t + 1) * LANES)
            total = buf[x, :, cols] + buf[x + 2, :, cols]
            total += jnp.where(row == 0, ylo[:, cols], pltpu.roll(c, 1, 0))
            total += jnp.where(row == by - 1, yhi[:, cols], pltpu.roll(c, by - 1, 0))
            total += jnp.where(lane == 0, shift_up[t - 1] if t > 0 else sides, shift_up[t])
            total += jnp.where(lane == LANES - 1, down[t + 1] if t + 1 < len(tiles) else sides, down[t])
            out.append(total)
        return v, jnp.concatenate(out, axis=1)

    for c in copies_g:
        c.wait()
    zp[0] = lax.fori_loop(0, bx, lambda x, acc: pack_plane(x, g[x + 1], 0, acc), zero_acc, unroll=8)
    pl.semaphore_wait(barrier, ndev - 1)
    faces0 = face_copies(0, g)
    for c in faces0:
        c.start()
    for c in copies_r:
        c.wait()
    for c in faces0:
        c.wait_recv()

    def residual_four(i, carry):
        acc, sides = carry
        total = jnp.zeros((by, bz), jnp.float32)
        for a in range(COARSEN):
            x = i * COARSEN + a
            v, around = plane_sum(x, g, 0, sides)
            sides = unpack_next(sides)
            res = rs[x] - (DIAG * v - around)
            r[x + 1] = res
            total += res
            acc = pack_plane(x, res, 1, acc)
        pooled[i] = total
        return acc, sides

    acc, _ = lax.fori_loop(0, q.cx, residual_four, (zero_acc, unpack_start(0)))
    zp[1] = acc
    for c in copies_t:
        c.wait()

    def fold_rows(i, carry):
        rows16[i] = dot(pool[...], pooled[i])
        return carry

    lax.fori_loop(0, q.cx, fold_rows, 0, unroll=True)
    cells = rows16[...].reshape(q.cx * q.cy, bz)
    first[...] = dot(cells, mz[iz]).reshape(first.shape)

    def spread_out(src, dst, stage, peers, here, device_of, own):
        def send(k, carry):
            d = (here + k) % peers
            pltpu.make_async_remote_copy(
                src_ref=src.at[d], dst_ref=dst.at[here], send_sem=a_send.at[stage], recv_sem=a_recv.at[stage],
                device_id=device_of(d), device_id_type=MESH,
            ).start()
            return carry

        lax.fori_loop(1, peers, send, 0)
        dst[here] = own

    def all_bytes(dst, count, sem):
        part = dst.at[pl.ds(0, count)]
        pltpu.make_async_copy(part, part, sem).wait()

    in_group = lambda d: (ix, d // q.pz, d % q.pz)
    spread_out(first, r1, 0, group, me_p, in_group, first[me_p])
    faces1 = face_copies(1, r)
    for c in faces1:
        c.start()

    def fix_planes(start, stop, carry):
        def body(i, carry):
            acc, sides = carry
            for a in range(COARSEN):
                x = i * COARSEN + a
                v, around = plane_sum(x, r, 1, sides)
                sides = unpack_next(sides)
                out = g[x + 1] + (v + around * (1.0 / DIAG)) * (1.0 / DIAG)
                u[x + 1] = out
                acc = pack_plane(x, out, 2, acc)
            return acc, sides

        return lax.fori_loop(start, stop, body, carry)

    all_bytes(r1, group - 1, a_recv.at[0])
    lines = dot(my[...], r1[...].reshape(group * q.rx * q.cy, q.lz))
    for d in range(ndev):
        s2[d] = lines[d * q.rows : (d + 1) * q.rows]
    spread_out(s2, r2, 1, ndev, me, coords, s2[me])
    for c in faces1:
        c.wait_recv()
    carry = fix_planes(0, q.cx // 2, (zero_acc, unpack_start(1)))
    all_bytes(r2, ndev - 1, a_recv.at[1])
    for d in range(ndev):
        flat[d * q.rows : (d + 1) * q.rows] = r2[d]
    spec = dot(mx[...], flat[...])
    spec = jnp.concatenate(
        [spec[k * q.lx : (k + 1) * q.lx] / (ei[...] + ey[me * q.rk + k]) for k in range(q.rk)], axis=0
    )
    lines = dot(mxi[...], spec)
    for d in range(ndev):
        s3[d] = lines[d * q.rows : (d + 1) * q.rows]
    spread_out(s3, r3, 2, ndev, me, coords, s3[me])
    zp[2] = fix_planes(q.cx // 2, q.cx, carry)[0]
    faces2 = face_copies(2, u)
    for c in faces2:
        c.start()
    all_bytes(r3, ndev - 1, a_recv.at[2])
    for d in range(ndev):
        flat[d * q.rows : (d + 1) * q.rows] = r3[d]
    s4[...] = dot(myi[...], flat[...]).reshape(s4.shape)

    def send_lines(k, carry):
        d = (me_p + k) % group
        pltpu.make_async_remote_copy(
            src_ref=s4.at[d // q.pz], dst_ref=r4.at[pl.ds(1 + me_p * q.rx, q.rx)],
            send_sem=a_send.at[3], recv_sem=a_recv.at[3], device_id=in_group(d), device_id_type=MESH,
        ).start()
        return carry

    lax.fori_loop(1, group, send_lines, 0)
    r4[pl.ds(1 + me_p * q.rx, q.rx)] = s4[iy]

    def edge(to_x, j, slot, sem):
        def send(d, carry):
            pltpu.make_async_remote_copy(
                src_ref=s4.at[d // q.pz, j], dst_ref=r4.at[slot], send_sem=a_send.at[sem], recv_sem=a_recv.at[sem],
                device_id=(to_x, d // q.pz, d % q.pz), device_id_type=MESH,
            ).start()
            return carry

        lax.fori_loop(0, group, send, 0)

    @pl.when(me_p == group - 1)
    def _():
        edge((ix + 1) % q.px, q.rx - 1, 0, 4)

    @pl.when(me_p == 0)
    def _():
        edge((ix + q.px - 1) % q.px, 0, q.cx + 1, 5)

    for c in faces2:
        c.wait_recv()

    def before_four(i, sides):
        for a in range(COARSEN):
            x = i * COARSEN + a
            v, around = plane_sum(x, u, 2, sides)
            sides = unpack_next(sides)
            n[x] = rs[x] - (DIAG * v - around)
        return sides

    lax.fori_loop(0, q.cx, before_four, unpack_start(2))

    all_bytes(r4, (group - 1) * q.rx, a_recv.at[3])
    all_bytes(r4, 1, a_recv.at[4])
    all_bytes(r4, 1, a_recv.at[5])
    lines = r4[...].reshape((q.cx + 2) * q.hr, q.lz)
    zf[...] = dot(lines, mzi[2 * iz]).reshape(zf.shape)
    zs[...] = dot(lines[q.hr : -q.hr], mzi[2 * iz + 1]).reshape(zs.shape)

    def coarse_rows(i, carry):
        c = zf[i + 1]
        mid = c[: q.cy]
        co[i, 0] = mid
        co[i, 1] = (DIAG - 4.0) * mid - zs[i, : q.cy]
        co[i, 2] = mid - zf[i, : q.cy]
        co[i, 3] = mid - zf[i + 2, : q.cy]
        co[i, 4] = mid - jnp.concatenate([c[q.cy : q.cy + 1], c[: q.cy - 1]], axis=0)
        co[i, 5] = mid - jnp.concatenate([c[1 : q.cy], c[q.cy + 1 : q.cy + 2]], axis=0)
        return carry

    lax.fori_loop(0, q.cx, coarse_rows, 0, unroll=2)

    sub = lax.broadcasted_iota(jnp.int32, (8, bz), 0)
    first_half = sub < COARSEN

    def finish(i, total):
        for t in range(by // 8):
            def spread(slot):
                lo = jnp.broadcast_to(co[i, slot, 2 * t : 2 * t + 1], (8, bz))
                hi = jnp.broadcast_to(co[i, slot, 2 * t + 1 : 2 * t + 2], (8, bz))
                return jnp.where(first_half, lo, hi)

            ys = slice(8 * t, 8 * t + 8)
            p = spread(0)
            flat_part = spread(1)
            flat_part += jnp.where(sub % COARSEN == 0, spread(4), 0.0)
            flat_part += jnp.where(sub % COARSEN == COARSEN - 1, spread(5), 0.0)
            for a in range(COARSEN):
                x = i * COARSEN + a
                change = flat_part
                if a == 0:
                    change = change + spread(2)
                if a == COARSEN - 1:
                    change = change + spread(3)
                up[x, ys] = u[x + 1, ys] + p
                res = n[x, ys] - change
                n[x, ys] = res
                total += res * res
        return total

    total = lax.fori_loop(0, q.cx, finish, jnp.zeros((8, bz), jnp.float32))

    line = jnp.sum(total, axis=0, keepdims=True)
    part = line[:, :LANES]
    for t in range(1, bz // LANES):
        part = part + line[:, t * LANES : (t + 1) * LANES]
    nrm[me] = part

    def send_norm(k, carry):
        d = (me + k) % ndev
        pltpu.make_async_remote_copy(
            src_ref=nrm.at[me], dst_ref=nrm.at[me], send_sem=a_send.at[6], recv_sem=a_recv.at[6],
            device_id=coords(d), device_id_type=MESH,
        ).start()
        return carry

    lax.fori_loop(1, ndev, send_norm, 0)
    all_bytes(nrm, ndev - 1, a_recv.at[6])
    norm_out[...] = jnp.sqrt(jnp.sum(jnp.sum(nrm[...], axis=0), axis=1, keepdims=True)).reshape(1, 1)

    all_bytes(nrm, ndev - 1, a_send.at[6])
    all_bytes(first, group - 1, a_send.at[0])
    all_bytes(s2, ndev - 1, a_send.at[1])
    all_bytes(s3, ndev - 1, a_send.at[2])
    all_bytes(r4, (group - 1) * q.rx, a_send.at[3])

    @pl.when(me_p == group - 1)
    def _():
        all_bytes(r4, group, a_send.at[4])

    @pl.when(me_p == 0)
    def _():
        all_bytes(r4, group, a_send.at[5])

    for c in faces0 + faces1 + faces2:
        c.wait_send()


def per_device(right_side, guess):
    counts = tuple(lax.axis_size(a) for a in ("gx", "gy", "gz"))
    q = Plan(counts, guess.shape)
    assert q.lz == LANES and 2 * q.bx <= LANES and q.bz % LANES == 0 and q.by % 8 == 0
    tables = q.tables()
    f32 = jnp.float32
    bx, by, bz = guess.shape
    vm = lambda *shape: pltpu.VMEM(shape, f32)
    scratch = [vm(*t.shape) for t in tables] + [
        vm(bx, by, bz), vm(bx + 2, by, bz), vm(bx + 2, by, bz), vm(bx + 2, by, bz),
        vm(3, 2, bx, 1, bz), vm(3, by, LANES), vm(3, 2, bx, 1, bz), vm(3, 2, by, LANES),
        vm(q.cx, by, bz), vm(q.cx, q.cy, bz),
        vm(q.group, q.rx, q.cy, q.lz), vm(q.group, q.rx, q.cy, q.lz),
        vm(q.ndev, q.rows, q.lz), vm(q.ndev, q.rows, q.lz), vm(q.ndev * q.rows, q.lz),
        vm(q.ndev, q.rows, q.lz), vm(q.ndev, q.rows, q.lz),
        vm(q.py, q.rx, q.hr, q.lz), vm(q.cx + 2, q.hr, q.lz),
        vm(q.cx + 2, q.hr, bz), vm(q.cx, q.hr, bz), vm(q.cx, 6, q.cy, bz), vm(q.ndev, 1, LANES),
        pltpu.SemaphoreType.DMA((8,)), pltpu.SemaphoreType.DMA((len(tables),)),
        pltpu.SemaphoreType.DMA((3, 6)), pltpu.SemaphoreType.DMA((3, 6)),
        pltpu.SemaphoreType.DMA((7,)), pltpu.SemaphoreType.DMA((7,)),
    ]
    updated, new_residual, norm = pl.pallas_call(
        functools.partial(kernel, q),
        out_shape=[
            pltpu.VMEM(guess.shape, f32),
            pltpu.VMEM(guess.shape, f32),
            jax.ShapeDtypeStruct((1, 1), f32),
        ],
        in_specs=[pl.BlockSpec(memory_space=pl.ANY)] * (2 + len(tables)),
        out_specs=[
            pl.BlockSpec(memory_space=pltpu.VMEM),
            pl.BlockSpec(memory_space=pltpu.VMEM),
            pl.BlockSpec(memory_space=pltpu.VMEM),
        ],
        scratch_shapes=scratch,
        compiler_params=pltpu.CompilerParams(
            collective_id=0, has_side_effects=True, vmem_limit_bytes=57100 * 1024
        ),
        name="schwarz_step",
    )(right_side, guess, *[jnp.asarray(t) for t in tables])
    return updated, new_residual, norm[0, 0]


def solution(mesh):
    return jax.shard_map(
        per_device,
        mesh=mesh,
        in_specs=(P("gx", "gy", "gz"), P("gx", "gy", "gz")),
        out_specs=(P("gx", "gy", "gz"), P("gx", "gy", "gz"), P()),
        check_vma=False,
    )
```

```python
import functools

import jax
import jax.numpy as jnp
import numpy as np
from jax import lax
from jax.experimental import pallas as pl
from jax.experimental.pallas import tpu as pltpu
from jax.sharding import PartitionSpec as P

COARSEN = 4
SCREEN = 0.002
DIAG = 6.0 + SCREEN
LANES = 128
EXACT = lax.Precision.HIGHEST
MESH = pl.DeviceIdType.MESH


def cas(length):
    index = np.arange(length)
    angle = 2.0 * np.pi * (np.outer(index, index) % length) / length
    return np.cos(angle) + np.sin(angle)


def eigen_line(length):
    index = np.arange(length)
    return (2.0 - 2.0 * np.cos(2.0 * np.pi * index / length)) / (COARSEN * COARSEN)


class Plan:
    def __init__(self, counts, block):
        self.px, self.py, self.pz = counts
        self.bx, self.by, self.bz = block
        self.ndev = self.px * self.py * self.pz
        self.group = self.py * self.pz
        self.cx, self.cy, self.cz = (n // COARSEN for n in block)
        self.lx, self.ly, self.lz = self.cx * self.px, self.cy * self.py, self.cz * self.pz
        self.rx = self.cx // self.group
        self.rk = self.ly // self.ndev
        assert self.rx * self.group == self.cx and self.rk * self.ndev == self.ly
        self.rows = self.rx * self.rk
        self.hr = -(-(self.cy + 2) // 8) * 8

    def tables(self):
        px, py, pz, group, ndev = self.px, self.py, self.pz, self.group, self.ndev
        cx, cy, cz, rx, rk = self.cx, self.cy, self.cz, self.rx, self.rk
        lx, ly, lz, hr = self.lx, self.ly, self.lz, self.hr
        tx, ty, tz = cas(lx), cas(ly), cas(lz)
        up_z = np.arange(self.bz) // COARSEN
        mz = np.stack([tz[g * cz + up_z] for g in range(pz)]) / COARSEN**3
        pool = (np.arange(self.by)[None, :] // COARSEN == np.arange(cy)[:, None]) * 1.0
        my = np.zeros((ndev, rx, rk, py, pz, rx, cy))
        for j in range(rx):
            part = ty.reshape(py, cy, ndev, rk).transpose(2, 3, 0, 1)
            my[:, j, :, :, :, j, :] = part[:, :, :, None, :]
        my = my.reshape(ndev * rx * rk, group * rx * cy)
        mx = np.zeros((rk, lx, px, group, rx, rk))
        for k in range(rk):
            mx[k, :, :, :, :, k] = tx.reshape(px, group, rx, lx).transpose(3, 0, 1, 2)
        mx = mx.reshape(rk * lx, ndev * rx * rk)
        mxi = mx.T / (lx * ly * lz)
        rows_of = np.arange(py)[:, None] * cy + np.concatenate([np.arange(cy), [-1, cy]])[None, :]
        lines = np.zeros((py, hr, ly))
        lines[:, : cy + 2] = ty[rows_of % ly]
        myi = np.zeros((py, rx, hr, ndev, rx, rk))
        for j in range(rx):
            myi[:, j, :, :, j, :] = lines.reshape(py, hr, ndev, rk)
        myi = myi.reshape(py * rx * hr, ndev * rx * rk)
        fine_z = np.arange(self.bz * pz) // COARSEN
        own, around = tz[:, fine_z], tz[:, np.roll(fine_z, 1)] + tz[:, np.roll(fine_z, -1)]
        mzi = np.stack([m[:, g * self.bz : (g + 1) * self.bz] for g in range(pz) for m in (own, around)])
        ei = SCREEN + eigen_line(lx)[:, None] + eigen_line(lz)[None, :]
        ey = np.repeat(eigen_line(ly)[:, None, None], lz, axis=2)
        return [t.astype(np.float32) for t in (mz, pool, my, mx, mxi, myi, mzi, ei, ey)]


def dot(a, b):
    return jnp.dot(a, b, precision=EXACT, preferred_element_type=jnp.float32)


def kernel(plan, rs_hbm, g_hbm, *refs):
    q = plan
    table_hbm = refs[:9]
    up, n, norm_out = refs[9:12]
    tabs = refs[12:21]
    mz, pool, my, mx, mxi, myi, mzi, ei, ey = tabs
    (rs, g, r, u, yp, zp, yh, zh, pooled, rows16, first, r1, s2, r2, flat, s3, r3, s4, r4, zf, zs, co, nrm,
     in_sem, tab_sem, face_send, face_recv, a_send, a_recv) = refs[21:]
    ndev, group = q.ndev, q.group
    bx, by, bz = q.bx, q.by, q.bz
    ix, iy, iz = lax.axis_index("gx"), lax.axis_index("gy"), lax.axis_index("gz")
    me_p = iy * q.pz + iz
    me = ix * group + me_p

    def wrapped(i, count):
        return [i] + [jnp.where(i + d >= count, i + d - count, i + d) for d in range(1, count)]

    xs, ys_, zs_ = wrapped(ix, q.px), wrapped(iy, q.py), wrapped(iz, q.pz)
    far_first = sorted(range(q.px), key=lambda d: -min(d, q.px - d))
    group_peers = [(ix, b, c) for b in reversed(ys_) for c in reversed(zs_)][: group - 1]
    all_peers = [(xs[a], b, c) for a in far_first for b in reversed(ys_) for c in reversed(zs_)][: ndev - 1]

    in_chunks = 4
    step = bx // in_chunks
    copies_g = [
        pltpu.make_async_copy(g_hbm.at[pl.ds(c * step, step)], g.at[pl.ds(1 + c * step, step)], in_sem.at[c])
        for c in range(in_chunks)
    ]
    copies_r = [
        pltpu.make_async_copy(rs_hbm.at[pl.ds(c * step, step)], rs.at[pl.ds(c * step, step)], in_sem.at[in_chunks + c])
        for c in range(in_chunks)
    ]
    copies_t = [pltpu.make_async_copy(a, b, tab_sem.at[i]) for i, (a, b) in enumerate(zip(table_hbm, tabs))]
    for c in copies_g + copies_r + copies_t:
        c.start()

    barrier = pltpu.get_barrier_semaphore()

    for peer in all_peers:
        pl.semaphore_signal(barrier, inc=1, device_id=peer, device_id_type=MESH)

    lane = lax.broadcasted_iota(jnp.int32, (by, LANES), 1)
    row = lax.broadcasted_iota(jnp.int32, (by, LANES), 0)

    def pack_plane(x, v, phase, acc, back=0):
        yp[phase, 0, x] = v[0:1, :]
        yp[phase, 1, x] = v[by - 1 : by, :]
        edge = jnp.where(lane == 0, v[:, :LANES], v[:, bz - LANES :])
        to = (LANES - 2 * back) % LANES
        if back:
            edge = pltpu.roll(edge, to, 1)
        return jnp.where((lane == to) | (lane == (to + LANES - 1) % LANES), edge, acc)

    def pack_next(acc, planes):
        return pltpu.roll(acc, LANES - 2 * planes, 1)

    def unpack_start(phase):
        left, right = zh[phase, 0], zh[phase, 0 if q.pz == 2 else 1]
        left = pltpu.roll(left, (2 * bx - 1) % LANES, 1)
        right = pltpu.roll(right, (2 * bx - 3) % LANES, 1)
        return jnp.where(lane % 2 == 0, left, right)

    def ahead(sides, planes):
        return pltpu.roll(sides, LANES - 2 * planes, 1) if planes else sides

    zero_acc = jnp.zeros((by, LANES), jnp.float32)

    def face_copies(phase, buf):
        xl, xr = (ix + q.px - 1) % q.px, (ix + 1) % q.px
        yl, yr = (iy + q.py - 1) % q.py, (iy + 1) % q.py
        zl, zr = (iz + q.pz - 1) % q.pz, (iz + 1) % q.pz
        moves = [
            (buf.at[1], buf.at[bx + 1], (xl, iy, iz)),
            (buf.at[bx], buf.at[0], (xr, iy, iz)),
            (yp.at[phase, 0], yh.at[phase, 1], (ix, yl, iz)),
            (yp.at[phase, 1], yh.at[phase, 0], (ix, yr, iz)),
            (zp.at[phase], zh.at[phase, 0], (ix, iy, zr)),
            (zp.at[phase], zh.at[phase, 1], (ix, iy, zl)),
        ]
        if q.pz == 2:
            moves.pop()
        return [
            pltpu.make_async_remote_copy(
                src_ref=s, dst_ref=d, send_sem=face_send.at[phase, i], recv_sem=face_recv.at[phase, i],
                device_id=dev, device_id_type=MESH,
            )
            for i, (s, d, dev) in enumerate(moves)
        ]

    def plane_sum(x, buf, phase, sides):
        v = buf[x + 1]
        ylo, yhi = yh[phase, 0, x], yh[phase, 1, x]
        tiles = [v[:, t * LANES : (t + 1) * LANES] for t in range(bz // LANES)]
        shift_up = [pltpu.roll(t, 1, 1) for t in tiles]
        down = [pltpu.roll(t, LANES - 1, 1) for t in tiles]
        out = []
        for t, c in enumerate(tiles):
            cols = slice(t * LANES, (t + 1) * LANES)
            total = buf[x, :, cols] + buf[x + 2, :, cols]
            total += jnp.where(row == 0, ylo[:, cols], pltpu.roll(c, 1, 0))
            total += jnp.where(row == by - 1, yhi[:, cols], pltpu.roll(c, by - 1, 0))
            total += jnp.where(lane == 0, shift_up[t - 1] if t > 0 else sides, shift_up[t])
            total += jnp.where(lane == LANES - 1, down[t + 1] if t + 1 < len(tiles) else sides, down[t])
            out.append(total)
        return v, jnp.concatenate(out, axis=1)

    for c in copies_g:
        c.wait()
    many = 4 * COARSEN

    def pack_many(i, acc):
        acc = pack_next(acc, many)
        for a in range(many):
            acc = pack_plane(i * many + a, g[i * many + a + 1], 0, acc, many - 1 - a)
        return acc

    zp[0] = lax.fori_loop(0, bx // many, pack_many, zero_acc)
    pl.semaphore_wait(barrier, ndev - 1)
    faces0 = face_copies(0, g)
    for c in faces0:
        c.start()
    for c in copies_r:
        c.wait()
    for c in faces0:
        c.wait_recv()

    def residual_four(i, carry):
        acc, sides = carry
        acc = pack_next(acc, COARSEN)
        total = jnp.zeros((by, bz), jnp.float32)
        for a in range(COARSEN):
            x = i * COARSEN + a
            v, around = plane_sum(x, g, 0, ahead(sides, a))
            res = rs[x] - (DIAG * v - around)
            r[x + 1] = res
            total += res
            acc = pack_plane(x, res, 1, acc, COARSEN - 1 - a)
        pooled[i] = total
        return acc, ahead(sides, COARSEN)

    acc, _ = lax.fori_loop(0, q.cx, residual_four, (zero_acc, unpack_start(0)))
    zp[1] = acc
    for c in copies_t:
        c.wait()

    def fold_rows(i, carry):
        rows16[i] = dot(pool[...], pooled[i])
        return carry

    lax.fori_loop(0, q.cx, fold_rows, 0, unroll=True)
    cells = rows16[...].reshape(q.cx * q.cy, bz)
    first[...] = dot(cells, mz[iz]).reshape(first.shape)

    def spread_out(src, dst, stage, peers, here, own):
        for px, py, pz in peers:
            d = py * q.pz + pz
            if len(peers) >= group:
                d = d + px * group
            pltpu.make_async_remote_copy(
                src_ref=src.at[d], dst_ref=dst.at[here], send_sem=a_send.at[stage], recv_sem=a_recv.at[stage],
                device_id=(px, py, pz), device_id_type=MESH,
            ).start()
        dst[here] = own

    def all_bytes(dst, count, sem):
        part = dst.at[pl.ds(0, count)]
        pltpu.make_async_copy(part, part, sem).wait()

    spread_out(first, r1, 0, group_peers, me_p, first[me_p])
    faces1 = face_copies(1, r)
    for c in faces1:
        c.start()

    def fix_planes(start, stop, carry):
        def body(i, carry):
            acc, sides = carry
            acc = pack_next(acc, COARSEN)
            for a in range(COARSEN):
                x = i * COARSEN + a
                v, around = plane_sum(x, r, 1, ahead(sides, a))
                out = g[x + 1] + (v + around * (1.0 / DIAG)) * (1.0 / DIAG)
                u[x + 1] = out
                acc = pack_plane(x, out, 2, acc, COARSEN - 1 - a)
            return acc, ahead(sides, COARSEN)

        return lax.fori_loop(start, stop, body, carry)

    all_bytes(r1, group - 1, a_recv.at[0])
    lines = dot(my[...], r1[...].reshape(group * q.rx * q.cy, q.lz))
    for d in range(ndev):
        s2[d] = lines[d * q.rows : (d + 1) * q.rows]
    spread_out(s2, r2, 1, all_peers, me, s2[me])
    for c in faces1:
        c.wait_recv()
    carry = fix_planes(0, q.cx // 2, (zero_acc, unpack_start(1)))
    all_bytes(r2, ndev - 1, a_recv.at[1])
    for d in range(ndev):
        flat[d * q.rows : (d + 1) * q.rows] = r2[d]
    spec = dot(mx[...], flat[...])
    spec = jnp.concatenate(
        [spec[k * q.lx : (k + 1) * q.lx] / (ei[...] + ey[me * q.rk + k]) for k in range(q.rk)], axis=0
    )
    lines = dot(mxi[...], spec)
    for d in range(ndev):
        s3[d] = lines[d * q.rows : (d + 1) * q.rows]
    spread_out(s3, r3, 2, all_peers, me, s3[me])
    zp[2] = fix_planes(q.cx // 2, q.cx, carry)[0]
    faces2 = face_copies(2, u)
    for c in faces2:
        c.start()
    all_bytes(r3, ndev - 1, a_recv.at[2])
    for d in range(ndev):
        flat[d * q.rows : (d + 1) * q.rows] = r3[d]
    s4[...] = dot(myi[...], flat[...]).reshape(s4.shape)

    for peer in group_peers:
        pltpu.make_async_remote_copy(
            src_ref=s4.at[peer[1]], dst_ref=r4.at[pl.ds(1 + me_p * q.rx, q.rx)],
            send_sem=a_send.at[3], recv_sem=a_recv.at[3], device_id=peer, device_id_type=MESH,
        ).start()
    r4[pl.ds(1 + me_p * q.rx, q.rx)] = s4[iy]

    def edge(to_x, j, slot, sem):
        def send(d, carry):
            pltpu.make_async_remote_copy(
                src_ref=s4.at[d // q.pz, j], dst_ref=r4.at[slot], send_sem=a_send.at[sem], recv_sem=a_recv.at[sem],
                device_id=(to_x, d // q.pz, d % q.pz), device_id_type=MESH,
            ).start()
            return carry

        lax.fori_loop(0, group, send, 0)

    @pl.when(me_p == group - 1)
    def _():
        edge((ix + 1) % q.px, q.rx - 1, 0, 4)

    @pl.when(me_p == 0)
    def _():
        edge((ix + q.px - 1) % q.px, 0, q.cx + 1, 5)

    for c in faces2:
        c.wait_recv()

    def before_four(i, sides):
        for a in range(COARSEN):
            x = i * COARSEN + a
            v, around = plane_sum(x, u, 2, ahead(sides, a))
            n[x] = rs[x] - (DIAG * v - around)
        return ahead(sides, COARSEN)

    lax.fori_loop(0, q.cx, before_four, unpack_start(2))

    all_bytes(r4, (group - 1) * q.rx, a_recv.at[3])
    all_bytes(r4, 1, a_recv.at[4])
    all_bytes(r4, 1, a_recv.at[5])
    lines = r4[...].reshape((q.cx + 2) * q.hr, q.lz)
    zf[...] = dot(lines, mzi[2 * iz]).reshape(zf.shape)
    zs[...] = dot(lines[q.hr : -q.hr], mzi[2 * iz + 1]).reshape(zs.shape)

    def coarse_rows(i, carry):
        c = zf[i + 1]
        mid = c[: q.cy]
        co[i, 0] = mid
        co[i, 1] = (DIAG - 4.0) * mid - zs[i, : q.cy]
        co[i, 2] = mid - zf[i, : q.cy]
        co[i, 3] = mid - zf[i + 2, : q.cy]
        co[i, 4] = mid - jnp.concatenate([c[q.cy : q.cy + 1], c[: q.cy - 1]], axis=0)
        co[i, 5] = mid - jnp.concatenate([c[1 : q.cy], c[q.cy + 1 : q.cy + 2]], axis=0)
        return carry

    lax.fori_loop(0, q.cx, coarse_rows, 0, unroll=2)

    sub = lax.broadcasted_iota(jnp.int32, (8, bz), 0)
    first_half = sub < COARSEN

    def spread(i, t, slot):
        lo = jnp.broadcast_to(co[i, slot, 2 * t : 2 * t + 1], (8, bz))
        hi = jnp.broadcast_to(co[i, slot, 2 * t + 1 : 2 * t + 2], (8, bz))
        return jnp.where(first_half, lo, hi)

    def finish(i, total):
        for t in range(by // 8):
            ys = slice(8 * t, 8 * t + 8)
            flat_part = spread(i, t, 1)
            flat_part += jnp.where(sub % COARSEN == 0, spread(i, t, 4), 0.0)
            flat_part += jnp.where(sub % COARSEN == COARSEN - 1, spread(i, t, 5), 0.0)
            for a in range(COARSEN):
                x = i * COARSEN + a
                change = flat_part
                if a == 0:
                    change = change + spread(i, t, 2)
                if a == COARSEN - 1:
                    change = change + spread(i, t, 3)
                res = n[x, ys] - change
                n[x, ys] = res
                total += res * res
        return total

    total = lax.fori_loop(0, q.cx, finish, jnp.zeros((8, bz), jnp.float32))

    line = jnp.sum(total, axis=0, keepdims=True)
    part = line[:, :LANES]
    for t in range(1, bz // LANES):
        part = part + line[:, t * LANES : (t + 1) * LANES]
    nrm[me] = part

    for peer in all_peers:
        pltpu.make_async_remote_copy(
            src_ref=nrm.at[me], dst_ref=nrm.at[me], send_sem=a_send.at[6], recv_sem=a_recv.at[6],
            device_id=peer, device_id_type=MESH,
        ).start()

    def finish_update(i, carry):
        for t in range(by // 8):
            ys = slice(8 * t, 8 * t + 8)
            p = spread(i, t, 0)
            for x in range(COARSEN):
                up[i * COARSEN + x, ys] = u[i * COARSEN + x + 1, ys] + p
        return carry

    lax.fori_loop(0, q.cx, finish_update, 0)
    all_bytes(nrm, ndev - 1, a_recv.at[6])
    norm_out[...] = jnp.sqrt(jnp.sum(jnp.sum(nrm[...], axis=0), axis=1, keepdims=True)).reshape(1, 1)

    all_bytes(nrm, ndev - 1, a_send.at[6])
    all_bytes(first, group - 1, a_send.at[0])
    all_bytes(s2, ndev - 1, a_send.at[1])
    all_bytes(s3, ndev - 1, a_send.at[2])
    all_bytes(r4, (group - 1) * q.rx, a_send.at[3])

    @pl.when(me_p == group - 1)
    def _():
        all_bytes(r4, group, a_send.at[4])

    @pl.when(me_p == 0)
    def _():
        all_bytes(r4, group, a_send.at[5])

    for c in faces0 + faces1 + faces2:
        c.wait_send()


def per_device(right_side, guess):
    counts = tuple(lax.axis_size(a) for a in ("gx", "gy", "gz"))
    q = Plan(counts, guess.shape)
    assert q.lz == LANES and 2 * q.bx <= LANES and q.bz % LANES == 0 and q.by % 8 == 0 and q.bx % 16 == 0
    tables = q.tables()
    f32 = jnp.float32
    bx, by, bz = guess.shape
    vm = lambda *shape: pltpu.VMEM(shape, f32)
    scratch = [vm(*t.shape) for t in tables] + [
        vm(bx, by, bz), vm(bx + 2, by, bz), vm(bx + 2, by, bz), vm(bx + 2, by, bz),
        vm(3, 2, bx, 1, bz), vm(3, by, LANES), vm(3, 2, bx, 1, bz), vm(3, 2, by, LANES),
        vm(q.cx, by, bz), vm(q.cx, q.cy, bz),
        vm(q.group, q.rx, q.cy, q.lz), vm(q.group, q.rx, q.cy, q.lz),
        vm(q.ndev, q.rows, q.lz), vm(q.ndev, q.rows, q.lz), vm(q.ndev * q.rows, q.lz),
        vm(q.ndev, q.rows, q.lz), vm(q.ndev, q.rows, q.lz),
        vm(q.py, q.rx, q.hr, q.lz), vm(q.cx + 2, q.hr, q.lz),
        vm(q.cx + 2, q.hr, bz), vm(q.cx, q.hr, bz), vm(q.cx, 6, q.cy, bz), vm(q.ndev, 1, LANES),
        pltpu.SemaphoreType.DMA((8,)), pltpu.SemaphoreType.DMA((len(tables),)),
        pltpu.SemaphoreType.DMA((3, 6)), pltpu.SemaphoreType.DMA((3, 6)),
        pltpu.SemaphoreType.DMA((7,)), pltpu.SemaphoreType.DMA((7,)),
    ]
    updated, new_residual, norm = pl.pallas_call(
        functools.partial(kernel, q),
        out_shape=[
            pltpu.VMEM(guess.shape, f32),
            pltpu.VMEM(guess.shape, f32),
            jax.ShapeDtypeStruct((1, 1), f32),
        ],
        in_specs=[pl.BlockSpec(memory_space=pl.ANY)] * (2 + len(tables)),
        out_specs=[
            pl.BlockSpec(memory_space=pltpu.VMEM),
            pl.BlockSpec(memory_space=pltpu.VMEM),
            pl.BlockSpec(memory_space=pltpu.VMEM),
        ],
        scratch_shapes=scratch,
        compiler_params=pltpu.CompilerParams(
            collective_id=0, has_side_effects=True, vmem_limit_bytes=57100 * 1024
        ),
        name="schwarz_step",
    )(right_side, guess, *[jnp.asarray(t) for t in tables])
    return updated, new_residual, norm[0, 0]


def solution(mesh):
    return jax.shard_map(
        per_device,
        mesh=mesh,
        in_specs=(P("gx", "gy", "gz"), P("gx", "gy", "gz")),
        out_specs=(P("gx", "gy", "gz"), P("gx", "gy", "gz"), P()),
        check_vma=False,
    )
```

```python
import functools

import jax
import jax.numpy as jnp
import numpy as np
from jax import lax
from jax.experimental import pallas as pl
from jax.experimental.pallas import tpu as pltpu
from jax.sharding import PartitionSpec as P

COARSEN = 4
SCREEN = 0.002
DIAG = 6.0 + SCREEN
LANES = 128
EXACT = lax.Precision.HIGHEST
MESH = pl.DeviceIdType.MESH


def cas(length):
    index = np.arange(length)
    angle = 2.0 * np.pi * (np.outer(index, index) % length) / length
    return np.cos(angle) + np.sin(angle)


def eigen_line(length):
    index = np.arange(length)
    return (2.0 - 2.0 * np.cos(2.0 * np.pi * index / length)) / (COARSEN * COARSEN)


class Plan:
    def __init__(self, counts, block):
        self.px, self.py, self.pz = counts
        self.bx, self.by, self.bz = block
        self.ndev = self.px * self.py * self.pz
        self.group = self.py * self.pz
        self.cx, self.cy, self.cz = (n // COARSEN for n in block)
        self.lx, self.ly, self.lz = self.cx * self.px, self.cy * self.py, self.cz * self.pz
        self.rx = self.cx // self.group
        self.rk = self.ly // self.ndev
        assert self.rx * self.group == self.cx and self.rk * self.ndev == self.ly
        self.rows = self.rx * self.rk
        self.hr = -(-(self.cy + 2) // 8) * 8

    def tables(self):
        px, py, pz, group, ndev = self.px, self.py, self.pz, self.group, self.ndev
        cx, cy, cz, rx, rk = self.cx, self.cy, self.cz, self.rx, self.rk
        lx, ly, lz, hr = self.lx, self.ly, self.lz, self.hr
        tx, ty, tz = cas(lx), cas(ly), cas(lz)
        up_z = np.arange(self.bz) // COARSEN
        mz = np.stack([tz[g * cz + up_z] for g in range(pz)]) / COARSEN**3
        pool = (np.arange(self.by)[None, :] // COARSEN == np.arange(cy)[:, None]) * 1.0
        my = np.zeros((ndev, rx, rk, py, pz, rx, cy))
        for j in range(rx):
            part = ty.reshape(py, cy, ndev, rk).transpose(2, 3, 0, 1)
            my[:, j, :, :, :, j, :] = part[:, :, :, None, :]
        my = my.reshape(ndev * rx * rk, group * rx * cy)
        mx = np.zeros((rk, lx, px, group, rx, rk))
        for k in range(rk):
            mx[k, :, :, :, :, k] = tx.reshape(px, group, rx, lx).transpose(3, 0, 1, 2)
        mx = mx.reshape(rk * lx, ndev * rx * rk)
        mxi = mx.T / (lx * ly * lz)
        rows_of = np.arange(py)[:, None] * cy + np.concatenate([np.arange(cy), [-1, cy]])[None, :]
        lines = np.zeros((py, hr, ly))
        lines[:, : cy + 2] = ty[rows_of % ly]
        myi = np.zeros((py, rx, hr, ndev, rx, rk))
        for j in range(rx):
            myi[:, j, :, :, j, :] = lines.reshape(py, hr, ndev, rk)
        myi = myi.reshape(py * rx * hr, ndev * rx * rk)
        fine_z = np.arange(self.bz * pz) // COARSEN
        own, around = tz[:, fine_z], tz[:, np.roll(fine_z, 1)] + tz[:, np.roll(fine_z, -1)]
        mzi = np.stack([m[:, g * self.bz : (g + 1) * self.bz] for g in range(pz) for m in (own, around)])
        ei = SCREEN + eigen_line(lx)[:, None] + eigen_line(lz)[None, :]
        ey = np.repeat(eigen_line(ly)[:, None, None], lz, axis=2)
        return [t.astype(np.float32) for t in (mz, pool, my, mx, mxi, myi, mzi, ei, ey)]


def dot(a, b):
    return jnp.dot(a, b, precision=EXACT, preferred_element_type=jnp.float32)


def kernel(plan, rs_hbm, g_hbm, *refs):
    q = plan
    table_hbm = refs[:9]
    up, n, norm_out = refs[9:12]
    tabs = refs[12:21]
    mz, pool, my, mx, mxi, myi, mzi, ei, ey = tabs
    (rs, g, r, u, yp, zp, yh, zh, pooled, rows16, first, r1, s2, r2, flat, s3, r3, s4, r4, zf, zs, co, nrm,
     in_sem, tab_sem, face_send, face_recv, a_send, a_recv) = refs[21:]
    ndev, group = q.ndev, q.group
    bx, by, bz = q.bx, q.by, q.bz
    ix, iy, iz = lax.axis_index("gx"), lax.axis_index("gy"), lax.axis_index("gz")
    me_p = iy * q.pz + iz
    me = ix * group + me_p

    def wrapped(i, count):
        return [i] + [jnp.where(i + d >= count, i + d - count, i + d) for d in range(1, count)]

    xs, ys_, zs_ = wrapped(ix, q.px), wrapped(iy, q.py), wrapped(iz, q.pz)
    far_first = sorted(range(q.px), key=lambda d: -min(d, q.px - d))
    group_peers = [(ix, b, c) for b in reversed(ys_) for c in reversed(zs_)][: group - 1]
    all_peers = [(xs[a], b, c) for a in far_first for b in reversed(ys_) for c in reversed(zs_)][: ndev - 1]

    in_chunks = min(4, q.bx // 16)
    step = bx // in_chunks
    copies_g = [
        pltpu.make_async_copy(g_hbm.at[pl.ds(c * step, step)], g.at[pl.ds(1 + c * step, step)], in_sem.at[c])
        for c in range(in_chunks)
    ]
    copies_r = [
        pltpu.make_async_copy(rs_hbm.at[pl.ds(c * step, step)], rs.at[pl.ds(c * step, step)], in_sem.at[in_chunks + c])
        for c in range(in_chunks)
    ]
    copies_t = [pltpu.make_async_copy(a, b, tab_sem.at[i]) for i, (a, b) in enumerate(zip(table_hbm, tabs))]
    for c in copies_g:
        c.start()

    barrier = pltpu.get_barrier_semaphore()

    for peer in all_peers:
        pl.semaphore_signal(barrier, inc=1, device_id=peer, device_id_type=MESH)

    lane = lax.broadcasted_iota(jnp.int32, (by, LANES), 1)
    row = lax.broadcasted_iota(jnp.int32, (by, LANES), 0)

    def pack_plane(x, v, phase, acc, back=0):
        yp[phase, 0, x] = v[0:1, :]
        yp[phase, 1, x] = v[by - 1 : by, :]
        edge = jnp.where(lane == 0, v[:, :LANES], v[:, bz - LANES :])
        to = (LANES - 2 * back) % LANES
        if back:
            edge = pltpu.roll(edge, to, 1)
        return jnp.where((lane == to) | (lane == (to + LANES - 1) % LANES), edge, acc)

    def pack_next(acc, planes):
        return pltpu.roll(acc, LANES - 2 * planes, 1)

    def unpack_start(phase):
        left, right = zh[phase, 0], zh[phase, 0 if q.pz == 2 else 1]
        left = pltpu.roll(left, (2 * bx - 1) % LANES, 1)
        right = pltpu.roll(right, (2 * bx - 3) % LANES, 1)
        return jnp.where(lane % 2 == 0, left, right)

    def ahead(sides, planes):
        return pltpu.roll(sides, LANES - 2 * planes, 1) if planes else sides

    zero_acc = jnp.zeros((by, LANES), jnp.float32)

    def face_copies(phase, buf):
        xl, xr = (ix + q.px - 1) % q.px, (ix + 1) % q.px
        yl, yr = (iy + q.py - 1) % q.py, (iy + 1) % q.py
        zl, zr = (iz + q.pz - 1) % q.pz, (iz + 1) % q.pz
        moves = [
            (buf.at[1], buf.at[bx + 1], (xl, iy, iz)),
            (buf.at[bx], buf.at[0], (xr, iy, iz)),
            (yp.at[phase, 0], yh.at[phase, 1], (ix, yl, iz)),
            (yp.at[phase, 1], yh.at[phase, 0], (ix, yr, iz)),
            (zp.at[phase], zh.at[phase, 0], (ix, iy, zr)),
            (zp.at[phase], zh.at[phase, 1], (ix, iy, zl)),
        ]
        if q.pz == 2:
            moves.pop()
        return [
            pltpu.make_async_remote_copy(
                src_ref=s, dst_ref=d, send_sem=face_send.at[phase, i], recv_sem=face_recv.at[phase, i],
                device_id=dev, device_id_type=MESH,
            )
            for i, (s, d, dev) in enumerate(moves)
        ]

    def plane_sum(x, buf, phase, sides):
        v = buf[x + 1]
        ylo, yhi = yh[phase, 0, x], yh[phase, 1, x]
        tiles = [v[:, t * LANES : (t + 1) * LANES] for t in range(bz // LANES)]
        shift_up = [pltpu.roll(t, 1, 1) for t in tiles]
        down = [pltpu.roll(t, LANES - 1, 1) for t in tiles]
        out = []
        for t, c in enumerate(tiles):
            cols = slice(t * LANES, (t + 1) * LANES)
            total = buf[x, :, cols] + buf[x + 2, :, cols]
            total += jnp.where(row == 0, ylo[:, cols], pltpu.roll(c, 1, 0))
            total += jnp.where(row == by - 1, yhi[:, cols], pltpu.roll(c, by - 1, 0))
            total += jnp.where(lane == 0, shift_up[t - 1] if t > 0 else sides, shift_up[t])
            total += jnp.where(lane == LANES - 1, down[t + 1] if t + 1 < len(tiles) else sides, down[t])
            out.append(total)
        return v, jnp.concatenate(out, axis=1)

    many = 16

    def pack_planes(buf, phase, start, stop, acc):
        def body(i, acc):
            acc = pack_next(acc, many)
            for a in range(many):
                acc = pack_plane(i * many + a, buf[i * many + a + 1], phase, acc, many - 1 - a)
            return acc

        return lax.fori_loop(start // many, stop // many, body, acc)

    acc = zero_acc
    for i, c in enumerate(copies_g):
        c.wait()
        if i == in_chunks - 1:
            for other in copies_r + copies_t:
                other.start()
        acc = pack_planes(g, 0, i * step, (i + 1) * step, acc)
    zp[0] = acc
    pl.semaphore_wait(barrier, ndev - 1)
    faces0 = face_copies(0, g)
    for c in faces0:
        c.start()
    for c in copies_r:
        c.wait()
    for c in faces0:
        c.wait_recv()

    def residual_four(i, carry):
        sides = carry
        total = jnp.zeros((by, bz), jnp.float32)
        for a in range(COARSEN):
            x = i * COARSEN + a
            v, around = plane_sum(x, g, 0, ahead(sides, a))
            res = rs[x] - (DIAG * v - around)
            r[x + 1] = res
            total += res
        pooled[i] = total
        return ahead(sides, COARSEN)

    lax.fori_loop(0, q.cx, residual_four, unpack_start(0))
    for c in copies_t:
        c.wait()

    def fold_rows(i, carry):
        rows16[i] = dot(pool[...], pooled[i])
        return carry

    lax.fori_loop(0, q.cx, fold_rows, 0, unroll=True)
    cells = rows16[...].reshape(q.cx * q.cy, bz)
    first[...] = dot(cells, mz[iz]).reshape(first.shape)

    def spread_out(src, dst, stage, peers, here, own):
        for px, py, pz in peers:
            d = py * q.pz + pz
            if len(peers) >= group:
                d = d + px * group
            pltpu.make_async_remote_copy(
                src_ref=src.at[d], dst_ref=dst.at[here], send_sem=a_send.at[stage], recv_sem=a_recv.at[stage],
                device_id=(px, py, pz), device_id_type=MESH,
            ).start()
        dst[here] = own

    def all_bytes(dst, count, sem):
        part = dst.at[pl.ds(0, count)]
        pltpu.make_async_copy(part, part, sem).wait()

    spread_out(first, r1, 0, group_peers, me_p, first[me_p])
    zp[1] = pack_planes(r, 1, 0, bx, zero_acc)
    faces1 = face_copies(1, r)
    for c in faces1:
        c.start()

    def fix_planes(start, stop, sides):
        def body(i, sides):
            for a in range(COARSEN):
                x = i * COARSEN + a
                v, around = plane_sum(x, r, 1, ahead(sides, a))
                out = g[x + 1] + (v + around * (1.0 / DIAG)) * (1.0 / DIAG)
                u[x + 1] = out
            return ahead(sides, COARSEN)

        return lax.fori_loop(start, stop, body, sides)

    all_bytes(r1, group - 1, a_recv.at[0])
    lines = dot(my[...], r1[...].reshape(group * q.rx * q.cy, q.lz))
    for d in range(ndev):
        s2[d] = lines[d * q.rows : (d + 1) * q.rows]
    spread_out(s2, r2, 1, all_peers, me, s2[me])
    for c in faces1:
        c.wait_recv()
    sides = fix_planes(0, q.cx * 7 // 8, unpack_start(1))
    all_bytes(r2, ndev - 1, a_recv.at[1])
    for d in range(ndev):
        flat[d * q.rows : (d + 1) * q.rows] = r2[d]
    spec = dot(mx[...], flat[...])
    spec = jnp.concatenate(
        [spec[k * q.lx : (k + 1) * q.lx] / (ei[...] + ey[me * q.rk + k]) for k in range(q.rk)], axis=0
    )
    lines = dot(mxi[...], spec)
    for d in range(ndev):
        s3[d] = lines[d * q.rows : (d + 1) * q.rows]
    spread_out(s3, r3, 2, all_peers, me, s3[me])
    fix_planes(q.cx * 7 // 8, q.cx, sides)
    zp[2] = pack_planes(u, 2, 0, bx, zero_acc)
    faces2 = face_copies(2, u)
    for c in faces2:
        c.start()
    all_bytes(r3, ndev - 1, a_recv.at[2])
    for d in range(ndev):
        flat[d * q.rows : (d + 1) * q.rows] = r3[d]
    s4[...] = dot(myi[...], flat[...]).reshape(s4.shape)

    for peer in group_peers:
        pltpu.make_async_remote_copy(
            src_ref=s4.at[peer[1]], dst_ref=r4.at[pl.ds(1 + me_p * q.rx, q.rx)],
            send_sem=a_send.at[3], recv_sem=a_recv.at[3], device_id=peer, device_id_type=MESH,
        ).start()
    r4[pl.ds(1 + me_p * q.rx, q.rx)] = s4[iy]

    def edge(to_x, j, slot, sem):
        def send(d, carry):
            pltpu.make_async_remote_copy(
                src_ref=s4.at[d // q.pz, j], dst_ref=r4.at[slot], send_sem=a_send.at[sem], recv_sem=a_recv.at[sem],
                device_id=(to_x, d // q.pz, d % q.pz), device_id_type=MESH,
            ).start()
            return carry

        lax.fori_loop(0, group, send, 0)

    @pl.when(me_p == group - 1)
    def _():
        edge((ix + 1) % q.px, q.rx - 1, 0, 4)

    @pl.when(me_p == 0)
    def _():
        edge((ix + q.px - 1) % q.px, 0, q.cx + 1, 5)

    for c in faces2:
        c.wait_recv()

    def before_four(i, sides):
        for a in range(COARSEN):
            x = i * COARSEN + a
            v, around = plane_sum(x, u, 2, ahead(sides, a))
            n[x] = rs[x] - (DIAG * v - around)
        return ahead(sides, COARSEN)

    lax.fori_loop(0, q.cx, before_four, unpack_start(2))

    all_bytes(r4, (group - 1) * q.rx, a_recv.at[3])
    all_bytes(r4, 1, a_recv.at[4])
    all_bytes(r4, 1, a_recv.at[5])
    lines = r4[...].reshape((q.cx + 2) * q.hr, q.lz)
    zf[...] = dot(lines, mzi[2 * iz]).reshape(zf.shape)
    zs[...] = dot(lines[q.hr : -q.hr], mzi[2 * iz + 1]).reshape(zs.shape)

    def coarse_rows(i, carry):
        c = zf[i + 1]
        mid = c[: q.cy]
        co[i, 0] = mid
        co[i, 1] = (DIAG - 4.0) * mid - zs[i, : q.cy]
        co[i, 2] = mid - zf[i, : q.cy]
        co[i, 3] = mid - zf[i + 2, : q.cy]
        co[i, 4] = mid - jnp.concatenate([c[q.cy : q.cy + 1], c[: q.cy - 1]], axis=0)
        co[i, 5] = mid - jnp.concatenate([c[1 : q.cy], c[q.cy + 1 : q.cy + 2]], axis=0)
        return carry

    lax.fori_loop(0, q.cx, coarse_rows, 0, unroll=2)

    sub = lax.broadcasted_iota(jnp.int32, (8, bz), 0)
    first_half = sub < COARSEN

    def spread(i, t, slot):
        lo = jnp.broadcast_to(co[i, slot, 2 * t : 2 * t + 1], (8, bz))
        hi = jnp.broadcast_to(co[i, slot, 2 * t + 1 : 2 * t + 2], (8, bz))
        return jnp.where(first_half, lo, hi)

    def finish(i, total):
        for t in range(by // 8):
            ys = slice(8 * t, 8 * t + 8)
            flat_part = spread(i, t, 1)
            flat_part += jnp.where(sub % COARSEN == 0, spread(i, t, 4), 0.0)
            flat_part += jnp.where(sub % COARSEN == COARSEN - 1, spread(i, t, 5), 0.0)
            for a in range(COARSEN):
                x = i * COARSEN + a
                change = flat_part
                if a == 0:
                    change = change + spread(i, t, 2)
                if a == COARSEN - 1:
                    change = change + spread(i, t, 3)
                res = n[x, ys] - change
                n[x, ys] = res
                total += res * res
        return total

    total = lax.fori_loop(0, q.cx, finish, jnp.zeros((8, bz), jnp.float32))

    line = jnp.sum(total, axis=0, keepdims=True)
    part = line[:, :LANES]
    for t in range(1, bz // LANES):
        part = part + line[:, t * LANES : (t + 1) * LANES]
    nrm[me] = part

    for peer in all_peers:
        pltpu.make_async_remote_copy(
            src_ref=nrm.at[me], dst_ref=nrm.at[me], send_sem=a_send.at[6], recv_sem=a_recv.at[6],
            device_id=peer, device_id_type=MESH,
        ).start()

    def finish_update(i, carry):
        for t in range(by // 8):
            ys = slice(8 * t, 8 * t + 8)
            p = spread(i, t, 0)
            for x in range(COARSEN):
                up[i * COARSEN + x, ys] = u[i * COARSEN + x + 1, ys] + p
        return carry

    lax.fori_loop(0, q.cx, finish_update, 0)
    all_bytes(nrm, ndev - 1, a_recv.at[6])
    norm_out[...] = jnp.sqrt(jnp.sum(jnp.sum(nrm[...], axis=0), axis=1, keepdims=True)).reshape(1, 1)

    all_bytes(nrm, ndev - 1, a_send.at[6])
    all_bytes(first, group - 1, a_send.at[0])
    all_bytes(s2, ndev - 1, a_send.at[1])
    all_bytes(s3, ndev - 1, a_send.at[2])
    all_bytes(r4, (group - 1) * q.rx, a_send.at[3])

    @pl.when(me_p == group - 1)
    def _():
        all_bytes(r4, group, a_send.at[4])

    @pl.when(me_p == 0)
    def _():
        all_bytes(r4, group, a_send.at[5])

    for c in faces0 + faces1 + faces2:
        c.wait_send()


def per_device(right_side, guess):
    counts = tuple(lax.axis_size(a) for a in ("gx", "gy", "gz"))
    q = Plan(counts, guess.shape)
    assert q.lz == LANES and 2 * q.bx <= LANES and q.bz % LANES == 0 and q.by % 8 == 0 and q.bx % 16 == 0
    tables = q.tables()
    f32 = jnp.float32
    bx, by, bz = guess.shape
    vm = lambda *shape: pltpu.VMEM(shape, f32)
    scratch = [vm(*t.shape) for t in tables] + [
        vm(bx, by, bz), vm(bx + 2, by, bz), vm(bx + 2, by, bz), vm(bx + 2, by, bz),
        vm(3, 2, bx, 1, bz), vm(3, by, LANES), vm(3, 2, bx, 1, bz), vm(3, 2, by, LANES),
        vm(q.cx, by, bz), vm(q.cx, q.cy, bz),
        vm(q.group, q.rx, q.cy, q.lz), vm(q.group, q.rx, q.cy, q.lz),
        vm(q.ndev, q.rows, q.lz), vm(q.ndev, q.rows, q.lz), vm(q.ndev * q.rows, q.lz),
        vm(q.ndev, q.rows, q.lz), vm(q.ndev, q.rows, q.lz),
        vm(q.py, q.rx, q.hr, q.lz), vm(q.cx + 2, q.hr, q.lz),
        vm(q.cx + 2, q.hr, bz), vm(q.cx, q.hr, bz), vm(q.cx, 6, q.cy, bz), vm(q.ndev, 1, LANES),
        pltpu.SemaphoreType.DMA((8,)), pltpu.SemaphoreType.DMA((len(tables),)),
        pltpu.SemaphoreType.DMA((3, 6)), pltpu.SemaphoreType.DMA((3, 6)),
        pltpu.SemaphoreType.DMA((7,)), pltpu.SemaphoreType.DMA((7,)),
    ]
    updated, new_residual, norm = pl.pallas_call(
        functools.partial(kernel, q),
        out_shape=[
            pltpu.VMEM(guess.shape, f32),
            pltpu.VMEM(guess.shape, f32),
            jax.ShapeDtypeStruct((1, 1), f32),
        ],
        in_specs=[pl.BlockSpec(memory_space=pl.ANY)] * (2 + len(tables)),
        out_specs=[
            pl.BlockSpec(memory_space=pltpu.VMEM),
            pl.BlockSpec(memory_space=pltpu.VMEM),
            pl.BlockSpec(memory_space=pltpu.VMEM),
        ],
        scratch_shapes=scratch,
        compiler_params=pltpu.CompilerParams(
            collective_id=0, has_side_effects=True, vmem_limit_bytes=57100 * 1024
        ),
        name="schwarz_step",
    )(right_side, guess, *[jnp.asarray(t) for t in tables])
    return updated, new_residual, norm[0, 0]


def solution(mesh):
    return jax.shard_map(
        per_device,
        mesh=mesh,
        in_specs=(P("gx", "gy", "gz"), P("gx", "gy", "gz")),
        out_specs=(P("gx", "gy", "gz"), P("gx", "gy", "gz"), P()),
        check_vma=False,
    )
```
